32 devices in a mesh: seq: 8 (over y, x, core), tp: 4 (over z).
Axes of the slice: x: 2, y: 2, z: 4, core: 2. Of those that a mesh axis runs over, the one named last changes fastest.
Arguments:
- hidden_in: bfloat16 [4096, 2048], P('seq', 'tp'), may hold values from -60 to 60
- w_query: bfloat16 [2048, 2048], P(None, 'tp'), may hold values from -0.125 to 0.125
- w_key: bfloat16 [2048, 2048], P(None, 'tp'), may hold values from -0.125 to 0.125
- w_value: bfloat16 [2048, 2048], P(None, 'tp'), may hold values from -0.8984375 to 0.8984375
- w_pos: bfloat16 [2048, 2048], P(None, 'tp'), may hold values from -0.125 to 0.125
- w_out: bfloat16 [2048, 2048], P('tp'), may hold values from -0.125 to 0.125
- bias_content: float32 [16, 128], P('tp'), may hold values from -4 to 4
- bias_pos: float32 [16, 128], P('tp'), may hold values from -4 to 4
- norm_gain: float32 [2048], P('tp'), may hold values from 0.1 to 1.9
- norm_bias: float32 [2048], P('tp'), may hold values from -3 to 3
Outputs:
- hidden_out: bfloat16 [4096, 2048], P('seq', 'tp')
The draws below stay inside these ranges and needn't reach their ends.
All inputs are finite; a program needn't handle non-finite values.
Results may differ from the reference program's by a relative error of at most 0.014.
The reference program's roundings to bfloat16 on the way count: a program that leaves them out, or rounds other values in their place, can miss the bound.
Values may be sent and summed in bfloat16 or wider, within the bound.
No kernel may reach another device: no remote copies, remote signals or barrier semaphores. Data moves between devices by JAX's collectives and lax.ppermute only.
A program may use at most 128 MiB of HBM per device.

```python
import jax
import jax.numpy as jnp
from jax import lax

D = 2048
HEADS = 16
HEAD_DIM = 128
SEG = 512
TOKENS = 4096
N_SEQ = 8
N_TP = 4


def draw_hidden_in(key, part):
    first, second, third = jax.random.split(key, 3)
    base = jax.random.normal(first, (TOKENS, D), jnp.float32)
    columns = jnp.exp(jnp.log(3.0) * jnp.arange(D).astype(jnp.float32) / D)
    columns = columns * jax.random.uniform(second, (D,), jnp.float32, minval=0.7, maxval=1.4)
    rows = jnp.exp(jax.random.uniform(third, (TOKENS, 1), jnp.float32, minval=0.0, maxval=jnp.log(2.0)))
    value = base * rows * columns[None, :]
    return jnp.clip(value, -60.0, 60.0).astype(jnp.bfloat16)


def levels(own_key, dims, pieces, least, top_value):
    def one(dim, parts):
        heights = jax.random.uniform(jax.random.fold_in(jax.random.fold_in(own_key, 6), dim), (parts,), jnp.float32, least / len(pieces), top_value / len(pieces))
        return jnp.repeat(jnp.exp(heights), dims[dim] // parts).reshape((-1,) + (1,) * (len(dims) - dim - 1))

    gain = one(*pieces[0])
    for cut in pieces[1:]:
        gain = gain * one(*cut)
    return gain


def scatter_about(own_key, extent, deviation, bound, shards=(), held_as=jnp.bfloat16):
    values = jax.random.normal(own_key, extent, jnp.float32) * deviation
    if len(shards) > 0:
        values = levels(own_key, extent, shards, -0.22, 0.18) * values
    return jnp.clip(values, min=-bound, max=bound).astype(held_as)


def setup_inputs(seed: int = 0) -> dict:
    splits = jax.random.split(jax.random.key(seed), 11)
    hidden_in = draw_hidden_in(jax.random.fold_in(splits[10], 71), 0)
    w_query = scatter_about(splits[1], (D, HEADS * HEAD_DIM), D ** -0.5, 0.125, ((1, 4),))
    w_key = scatter_about(splits[2], (D, HEADS * HEAD_DIM), D ** -0.5, 0.125, ((1, 4),))
    w_value = scatter_about(splits[3], (D, HEADS * HEAD_DIM), 0.15, 0.8984375, ((1, 4),))
    w_pos = scatter_about(splits[4], (D, HEADS * HEAD_DIM), D ** -0.5, 0.125, ((1, 4),))
    w_out = scatter_about(splits[5], (HEADS * HEAD_DIM, D), (HEADS * HEAD_DIM) ** -0.5, 0.125, ((0, 4),))
    bias_content = scatter_about(splits[6], (HEADS, HEAD_DIM), 1.0, 4.0, ((0, 4),), jnp.float32)
    bias_pos = scatter_about(splits[7], (HEADS, HEAD_DIM), 1.0, 4.0, ((0, 4),), jnp.float32)
    norm_gain = jnp.clip(1.0 + 0.18 * jax.random.normal(splits[8], (D,), jnp.float32), 0.1, 1.9)
    norm_bias = scatter_about(splits[9], (D,), 0.5, 3.0, ((0, 4),), jnp.float32)
    return dict(hidden_in=hidden_in, w_query=w_query, w_key=w_key, w_value=w_value, w_pos=w_pos, w_out=w_out, bias_content=bias_content, bias_pos=bias_pos, norm_gain=norm_gain, norm_bias=norm_bias)


def relative_table(span, width):
    half = width // 2
    freq = jnp.exp(-jnp.log(10000.0) * jnp.arange(half).astype(jnp.float32) / half)
    distance = (span - 1 - jnp.arange(span)).astype(jnp.float32)
    angle = distance[:, None] * freq[None, :]
    return jnp.concatenate([jnp.sin(angle), jnp.cos(angle)], 1).astype(jnp.bfloat16)

def shift_rows(table, seg, span):
    heads = table.shape[0]
    padded = jnp.pad(table, ((0, 0), (0, 0), (0, 1)))
    flat = padded.reshape(heads, seg * (span + 1))
    return flat[:, seg - 1:seg - 1 + seg * span].reshape(heads, seg, span)

def reference(hidden_in, w_query, w_key, w_value, w_pos, w_out, bias_content, bias_pos, norm_gain, norm_bias):
    span = 3 * SEG
    memory = 2 * SEG
    width = HEADS * HEAD_DIM
    query = jnp.dot(hidden_in, w_query, preferred_element_type=jnp.float32).astype(jnp.bfloat16)
    keys = jnp.dot(hidden_in, w_key, preferred_element_type=jnp.float32).astype(jnp.bfloat16)
    values = jnp.dot(hidden_in, w_value, preferred_element_type=jnp.float32).astype(jnp.bfloat16)
    rel = jnp.dot(relative_table(span, D), w_pos, preferred_element_type=jnp.float32).astype(jnp.bfloat16)
    rel = rel.reshape(span, HEADS, HEAD_DIM).astype(jnp.float32)
    front = jnp.zeros((memory, width), jnp.bfloat16)
    pad_keys = jnp.concatenate([front, keys], 0)
    pad_values = jnp.concatenate([front, values], 0)
    scale = 1.0 / jnp.sqrt(jnp.float32(HEAD_DIM))

    def one_segment(index):
        start = (index * SEG).astype(jnp.int32)
        q_rows = lax.dynamic_slice_in_dim(query, start, SEG, 0).astype(jnp.float32).reshape(SEG, HEADS, HEAD_DIM)
        k_rows = lax.dynamic_slice_in_dim(pad_keys, start, span, 0).astype(jnp.float32).reshape(span, HEADS, HEAD_DIM)
        v_rows = lax.dynamic_slice_in_dim(pad_values, start, span, 0).astype(jnp.float32).reshape(span, HEADS, HEAD_DIM)
        content_q = (q_rows + bias_content[None]).astype(jnp.bfloat16).astype(jnp.float32)
        pos_q = (q_rows + bias_pos[None]).astype(jnp.bfloat16).astype(jnp.float32)
        content = jnp.einsum('ihd,jhd->hij', content_q, k_rows)
        position = shift_rows(jnp.einsum('ihd,ehd->hie', pos_q, rel), SEG, span)
        score = (content + position) * scale
        row = jnp.arange(SEG)[:, None]
        col = jnp.arange(span)[None, :]
        allowed = (col <= row + memory) & (start - memory + col >= 0)
        score = jnp.where(allowed[None], score, jnp.float32(-1e+30))
        probs = jax.nn.softmax(score, axis=-1).astype(jnp.bfloat16).astype(jnp.float32)
        attended = jnp.einsum('hij,jhd->ihd', probs, v_rows)
        return attended.astype(jnp.bfloat16).reshape(SEG, width)
    attended = lax.map(one_segment, jnp.arange(N_SEQ).astype(jnp.int32)).reshape(TOKENS, width)
    group = width // N_TP
    branch = jnp.zeros((TOKENS, D), jnp.float32)
    for part in range(N_TP):
        piece = jnp.dot(attended[:, part * group:(part + 1) * group], w_out[part * group:(part + 1) * group], preferred_element_type=jnp.float32)
        branch = branch + piece.astype(jnp.bfloat16).astype(jnp.float32)
    summed = hidden_in.astype(jnp.float32) + branch
    center = lax.optimization_barrier(jnp.mean(summed, axis=1, keepdims=True))
    spread = lax.optimization_barrier(jnp.mean((summed - center) ** 2, axis=1, keepdims=True))
    normed = (summed - center) / jnp.sqrt(spread + 1e-05)
    return (normed * norm_gain[None] + norm_bias[None]).astype(jnp.bfloat16)
```

```python
import functools

import jax
import jax.numpy as jnp
from jax import lax
from jax.experimental import pallas as pl
from jax.experimental.pallas import tpu as pltpu
from jax.sharding import PartitionSpec as P

ROWS = 128


def relative_table(span, width):
    half = width // 2
    freq = jnp.exp(-jnp.log(10000.0) * jnp.arange(half).astype(jnp.float32) / half)
    distance = (span - 1 - jnp.arange(span)).astype(jnp.float32)
    angle = distance[:, None] * freq[None, :]
    return jnp.concatenate([jnp.sin(angle), jnp.cos(angle)], 1).astype(jnp.bfloat16)


def project_kernel(order, *refs, parts):
    hidden = refs[:parts]
    weights = refs[parts : parts + 3]
    outs = refs[parts + 3 : parts + 6]
    sums = refs[parts + 6 : parts + 9]
    step = pl.program_id(0)
    for part in range(parts):

        @pl.when(step == part)
        def _():
            block = hidden[part][...]
            for weight, total, out in zip(weights, sums, outs):
                value = jnp.dot(block, weight[...], preferred_element_type=jnp.float32)
                if part > 0:
                    value = total[...] + value
                if part < parts - 1:
                    total[...] = value
                else:
                    out[...] = value.astype(jnp.bfloat16)


def project(order, hidden, weights):
    parts = len(hidden)
    rows, block = hidden[0].shape
    width = weights[0].shape[1]
    grid_spec = pltpu.PrefetchScalarGridSpec(
        num_scalar_prefetch=1,
        grid=(parts,),
        in_specs=[pl.BlockSpec((rows, block), lambda k, o: (0, 0)) for _ in hidden]
        + [pl.BlockSpec((block, width), lambda k, o: (o[k], 0)) for _ in weights],
        out_specs=[pl.BlockSpec((rows, width), lambda k, o: (0, 0)) for _ in weights],
        scratch_shapes=[pltpu.VMEM((rows, width), jnp.float32) for _ in weights],
    )
    return pl.pallas_call(
        functools.partial(project_kernel, parts=parts),
        grid_spec=grid_spec,
        out_shape=[jax.ShapeDtypeStruct((rows, width), jnp.bfloat16) for _ in weights],
        cost_estimate=pl.CostEstimate(
            flops=6 * rows * parts * block * width,
            transcendentals=0,
            bytes_accessed=6 * parts * block * width,
        ),
        name="project",
    )(order, *hidden, *weights)


def attend_kernel(place, q, bias_c, bias_p, rel, *refs, first, counts, seg):
    parts = len(counts)
    keys = refs[:parts]
    values = refs[parts : 2 * parts]
    out = refs[2 * parts]
    head = pl.program_id(0)
    head_dim = q.shape[1]
    span = 3 * seg
    log2 = 1.4426950408889634 / head_dim**0.5
    content_bias = bias_c[pl.ds(head, 1), :]
    pos_bias = bias_p[pl.ds(head, 1), :]
    nt = (((1,), (1,)), ((), ()))
    for block in range(q.shape[0] // ROWS):
        top = first + block * ROWS
        width = 2 * seg + top + ROWS
        rows = q[block * ROWS : (block + 1) * ROWS, :].astype(jnp.float32)
        content_q = (rows + content_bias).astype(jnp.bfloat16)
        pos_q = (rows + pos_bias).astype(jnp.bfloat16)
        position = lax.dot_general(
            pos_q, rel[span - width :, :], nt, preferred_element_type=jnp.float32
        )
        position = pltpu.roll(position, width - (ROWS - 1), 1, stride=1, stride_axis=0)
        scores = []
        start = 0
        used = []
        for part in range(parts):
            count = min(counts[part], width - start)
            if count <= 0:
                break
            content = lax.dot_general(
                content_q, keys[part][:count, :], nt, preferred_element_type=jnp.float32
            )
            score = content + position[:, start : start + count]
            back = 2 - start // seg
            if back > 0:
                score = score + jnp.where(place[0] >= back, jnp.float32(0.0), jnp.float32(-1e30))
            if start + count == width:
                row = lax.broadcasted_iota(jnp.int32, (ROWS, ROWS), 0)
                col = lax.broadcasted_iota(jnp.int32, (ROWS, ROWS), 1)
                tail = jnp.where(col <= row, score[:, count - ROWS :], jnp.float32(-1e30))
                score = tail if count == ROWS else jnp.concatenate([score[:, : count - ROWS], tail], 1)
            scores.append(score)
            used.append(count)
            start += count
        score = jnp.concatenate(scores, 1)
        peak = jnp.max(score, axis=1, keepdims=True)
        weight = jnp.exp2((score - peak) * log2)
        total = jnp.sum(weight, axis=1, keepdims=True)
        probs = (weight * (1.0 / total)).astype(jnp.bfloat16)
        result = None
        start = 0
        for part, count in enumerate(used):
            piece = jnp.dot(
                probs[:, start : start + count],
                values[part][:count, :],
                preferred_element_type=jnp.float32,
            )
            result = piece if result is None else result + piece
            start += count
        out[block * ROWS : (block + 1) * ROWS, :] = result.astype(jnp.bfloat16)


def attend(place, query, bias_c, bias_p, rel, keys, values, first, seg):
    heads, head_dim = bias_c.shape
    counts = tuple(k.shape[0] for k in keys)
    rows = query.shape[0]
    column = lambda n: pl.BlockSpec((n, head_dim), lambda h, p: (0, h))
    whole = pl.BlockSpec((heads, head_dim), lambda h, p: (0, 0))
    grid_spec = pltpu.PrefetchScalarGridSpec(
        num_scalar_prefetch=1,
        grid=(heads,),
        in_specs=[column(rows), whole, whole, column(3 * seg)]
        + [column(n) for n in counts]
        + [column(n) for n in counts],
        out_specs=column(rows),
    )
    return pl.pallas_call(
        functools.partial(attend_kernel, first=first, counts=counts, seg=seg),
        grid_spec=grid_spec,
        out_shape=jax.ShapeDtypeStruct((rows, heads * head_dim), jnp.bfloat16),
        cost_estimate=pl.CostEstimate(
            flops=6 * rows * 3 * seg * heads * head_dim,
            transcendentals=rows * 3 * seg * heads,
            bytes_accessed=18 * seg * heads * head_dim,
        ),
        name="attend",
    )(place, query, bias_c, bias_p, rel, *keys, *values)


def shards(
    hidden_in, w_query, w_key, w_value, w_pos, w_out, bias_content, bias_pos, norm_gain, norm_bias
):
    seg, block = hidden_in.shape
    model_width = w_query.shape[0]
    span = 3 * seg
    tp = lax.axis_size("tp")
    seqs = lax.axis_size("seq")
    place = lax.axis_index("seq")
    rank = lax.axis_index("tp")

    def across(x, k):
        return lax.ppermute(x, "tp", [(i, i ^ k) for i in range(tp)])

    def later(x, k):
        return lax.ppermute(x, "seq", [(i, i + k) for i in range(seqs - k)])

    order = jnp.bitwise_xor(rank, jnp.arange(tp)).astype(jnp.int32)
    hidden = [hidden_in] + [across(hidden_in, k) for k in range(1, tp)]
    rel = jnp.dot(
        relative_table(span, model_width), w_pos, preferred_element_type=jnp.float32
    ).astype(jnp.bfloat16)
    query, own_keys, own_values = project(order, hidden, (w_query, w_key, w_value))
    keys = [later(own_keys, k) for k in (2, 1)] + [own_keys]
    values = [later(own_values, k) for k in (2, 1)] + [own_values]
    attended = attend(
        place.reshape(1).astype(jnp.int32), query, bias_content, bias_pos, rel, keys, values, 0, seg
    )
    partial_out = jnp.dot(attended, w_out, preferred_element_type=jnp.float32).astype(jnp.bfloat16)

    def columns(index):
        return lax.dynamic_slice_in_dim(partial_out, index * block, block, 1)

    summed = hidden_in.astype(jnp.float32) + columns(rank).astype(jnp.float32)
    for k in range(1, tp):
        summed = summed + across(columns(rank ^ k), k).astype(jnp.float32)
    total = jnp.sum(summed, axis=1)
    center = total / block
    centred = summed - center[:, None]
    spread = jnp.sum(centred * centred, axis=1)
    stats = jnp.stack([center, spread])
    stats = [stats] + [across(stats, k) for k in range(1, tp)]
    mean = sum(s[0] for s in stats) / tp
    spread = sum(s[1] + block * (s[0] - mean) ** 2 for s in stats) / model_width
    normed = (summed - mean[:, None]) / jnp.sqrt(spread[:, None] + 1e-05)
    return (normed * norm_gain[None] + norm_bias[None]).astype(jnp.bfloat16)


def solution(mesh):
    in_specs = (
        P("seq", "tp"),
        P(None, "tp"),
        P(None, "tp"),
        P(None, "tp"),
        P(None, "tp"),
        P("tp", None),
        P("tp", None),
        P("tp", None),
        P("tp"),
        P("tp"),
    )
    out_specs = P("seq", "tp")
    return jax.shard_map(shards, mesh=mesh, in_specs=in_specs, out_specs=out_specs, check_vma=False)
```

```python
import functools

import jax
import jax.numpy as jnp
from jax import lax
from jax.experimental import pallas as pl
from jax.experimental.pallas import tpu as pltpu
from jax.sharding import PartitionSpec as P

TILE = 128
ROWS = 256
HP = 2
VMEM = pltpu.CompilerParams(vmem_limit_bytes=16 * 2**20)
NT = (((1,), (1,)), ((), ()))
LOW = -1e30


def angles(distance, width):
    half = width // 2
    freq = jnp.exp(-jnp.log(10000.0) * jnp.arange(half).astype(jnp.float32) / half)
    angle = distance.astype(jnp.float32)[:, None] * freq[None, :]
    return jnp.sin(angle), jnp.cos(angle)


def relative_kernel(far_sin, far_cos, near_sin, near_cos, weight, out):
    block = pl.program_id(0)
    fs = far_sin[pl.ds(block, 1), :]
    fc = far_cos[pl.ds(block, 1), :]
    ns = near_sin[...]
    nc = near_cos[...]
    sin = (fs * nc + fc * ns).astype(jnp.bfloat16)
    cos = (fc * nc - fs * ns).astype(jnp.bfloat16)
    emb = jnp.concatenate([sin, cos], 1)
    out[...] = jnp.dot(emb, weight[...], preferred_element_type=jnp.float32).astype(jnp.bfloat16)


def relative(span, w_pos):
    model_width, width = w_pos.shape
    blocks = span // TILE
    far_sin, far_cos = angles(span - TILE - TILE * jnp.arange(blocks), model_width)
    near_sin, near_cos = angles(TILE - 1 - jnp.arange(TILE), model_width)
    whole = lambda a: pl.BlockSpec(a.shape, lambda b: (0, 0))
    return pl.pallas_call(
        relative_kernel,
        grid=(blocks,),
        in_specs=[whole(a) for a in (far_sin, far_cos, near_sin, near_cos, w_pos)],
        out_specs=pl.BlockSpec((TILE, width), lambda b: (b, 0)),
        out_shape=jax.ShapeDtypeStruct((span, width), jnp.bfloat16),
        compiler_params=VMEM,
        cost_estimate=pl.CostEstimate(
            flops=2 * span * model_width * width, transcendentals=0, bytes_accessed=4 * 2**20
        ),
        name="relative",
    )(far_sin, far_cos, near_sin, near_cos, w_pos)


def project_kernel(rank, own, one, two, near, relay, w_q, w_k, w_v, query, pairs, steps):
    block = own.shape[1]
    hidden = [own[...], one[...], two[...], near[...] + relay[...]]
    cols = query.shape[1]
    for weight, out in (
        (w_k, pairs.at[:, :cols]),
        (w_v, pairs.at[:, cols:]),
        (w_q, query),
    ):
        total = None
        for k, rows in enumerate(hidden):
            piece = weight[pl.ds(pl.multiple_of((rank[0] ^ k) * block, block), block), :]
            value = jnp.dot(rows, piece, preferred_element_type=jnp.float32)
            total = value if total is None else total + value
        out[...] = total.astype(jnp.bfloat16)


def project(rank, hidden, weights, steps=2):
    rows, block = hidden[0].shape
    depth, width = weights[0].shape
    cols = width // steps
    out_specs = [pl.BlockSpec((rows, cols), lambda n, o: (0, n)) for _ in range(3)]
    grid_spec = pltpu.PrefetchScalarGridSpec(
        num_scalar_prefetch=1,
        grid=(steps,),
        in_specs=[pl.BlockSpec((rows, block), lambda n, o: (0, 0)) for _ in hidden]
        + [pl.BlockSpec((depth, cols), lambda n, o: (0, n)) for _ in weights],
        out_specs=[
            pl.BlockSpec((rows, cols), lambda n, o: (0, n)),
            pl.BlockSpec((rows, 2 * cols), lambda n, o: (0, n)),
        ],
    )
    return pl.pallas_call(
        functools.partial(project_kernel, steps=steps),
        grid_spec=grid_spec,
        out_shape=[
            jax.ShapeDtypeStruct((rows, width), jnp.bfloat16),
            jax.ShapeDtypeStruct((rows, 2 * width), jnp.bfloat16),
        ],
        compiler_params=VMEM,
        cost_estimate=pl.CostEstimate(
            flops=6 * rows * depth * width, transcendentals=0, bytes_accessed=6 * depth * width
        ),
        name="project",
    )(rank, *hidden, *weights)


def attend_kernel(
    place, bias_c, bias_p, rel, *refs, first, count, pieces, seg, final, head_dim
):
    queries = refs[:count]
    pairs = refs[count : count + len(pieces)]
    refs = refs[count + len(pieces) :]
    wide = HP * head_dim
    span = 3 * seg
    log2 = 1.4426950408889634 / head_dim**0.5
    lane = lax.broadcasted_iota(jnp.int32, (ROWS, head_dim), 1)
    for local in range(HP):
        head = pl.program_id(0) * HP + local
        mine = slice(local * head_dim, (local + 1) * head_dim)
        theirs = slice(wide + local * head_dim, wide + (local + 1) * head_dim)
        content_bias = bias_c[pl.ds(head, 1), :]
        pos_bias = bias_p[pl.ds(head, 1), :]
        for block, q in enumerate(queries):
            here = slice(block * ROWS, (block + 1) * ROWS)
            top = first + block * ROWS
            end = 2 * seg + top + ROWS
            rows = q[:, mine].astype(jnp.float32)
            content_q = (rows + content_bias).astype(jnp.bfloat16)
            pos_q = (rows + pos_bias).astype(jnp.bfloat16)
            scores = []
            used = []
            for part, start in enumerate(pieces):
                width = min(pairs[part].shape[0], end - start)
                if width <= 0:
                    continue
                edge = start + width == end
                window = width if edge else width + ROWS
                low = seg - ROWS - top + start
                position = lax.dot_general(
                    pos_q, rel[low : low + window, mine], NT, preferred_element_type=jnp.float32
                )
                position = pltpu.roll(position, window - (ROWS - 1), 1, stride=1, stride_axis=0)
                content = lax.dot_general(
                    content_q, pairs[part][:width, mine], NT, preferred_element_type=jnp.float32
                )
                score = content + position[:, :width]
                back = 2 - start // seg
                if back > 0:
                    score = score + jnp.where(place[0] >= back, jnp.float32(0.0), jnp.float32(LOW))
                if edge:
                    row = lax.broadcasted_iota(jnp.int32, (ROWS, ROWS), 0)
                    col = lax.broadcasted_iota(jnp.int32, (ROWS, ROWS), 1)
                    tail = jnp.where(col <= row, score[:, width - ROWS :], jnp.float32(LOW))
                    score = tail if width == ROWS else jnp.concatenate([score[:, :-ROWS], tail], 1)
                scores.append(score)
                used.append((part, width))
            score = jnp.concatenate(scores, 1)
            peak = jnp.max(score, axis=1, keepdims=True)
            if final:
                before = refs[0][here, mine]
                old_peak = before[:, :1]
                old_total = before[:, head_dim // 2 : head_dim // 2 + 1]
                peak = jnp.maximum(peak, old_peak)
                keep = jnp.exp2((old_peak - peak) * log2)
            weight = jnp.exp2((score - peak) * log2)
            total = jnp.sum(weight, axis=1, keepdims=True)
            if final:
                total = total + old_total * keep
                scale = 1.0 / total
                weight = weight * scale
                result = refs[1][here, mine] * (keep * scale)
            else:
                result = None
            probs = weight.astype(jnp.bfloat16)
            start = 0
            for part, width in used:
                piece = jnp.dot(
                    probs[:, start : start + width],
                    pairs[part][:width, theirs],
                    preferred_element_type=jnp.float32,
                )
                result = piece if result is None else result + piece
                start += width
            if final:
                refs[2][here, mine] = result.astype(jnp.bfloat16)
            else:
                refs[0][here, mine] = jnp.where(lane < head_dim // 2, peak, total)
                refs[1][here, mine] = result


def attend(place, queries, bias_c, bias_p, rel, pairs, pieces, first, seg, before=()):
    heads, head_dim = bias_c.shape
    rows = len(queries) * ROWS
    wide = HP * head_dim
    final = len(before) > 0
    column = lambda n: pl.BlockSpec((n, wide), lambda h, p: (0, h))
    whole = pl.BlockSpec((heads, head_dim), lambda h, p: (0, 0))
    shape = lambda kind: jax.ShapeDtypeStruct((rows, heads * head_dim), kind)
    grid_spec = pltpu.PrefetchScalarGridSpec(
        num_scalar_prefetch=1,
        grid=(heads // HP,),
        in_specs=[whole, whole, column(3 * seg)]
        + [column(ROWS) for _ in queries]
        + [pl.BlockSpec((n.shape[0], 2 * wide), lambda h, p: (0, h)) for n in pairs]
        + [pl.BlockSpec((rows, wide), lambda h, p: (first // rows, h)) for _ in before],
        out_specs=column(rows) if final else [column(rows), column(rows)],
    )
    size = sum(k.shape[0] for k in pairs)
    return pl.pallas_call(
        functools.partial(
            attend_kernel,
            first=first,
            count=len(queries),
            pieces=pieces,
            seg=seg,
            final=final,
            head_dim=head_dim,
        ),
        grid_spec=grid_spec,
        out_shape=shape(jnp.bfloat16) if final else [shape(jnp.float32), shape(jnp.float32)],
        compiler_params=VMEM,
        cost_estimate=pl.CostEstimate(
            flops=16 * rows * size * heads * head_dim,
            transcendentals=rows * size * heads,
            bytes_accessed=6 * size * heads * head_dim,
        ),
        name="finish" if final else "begin",
    )(place, bias_c, bias_p, rel, *queries, *pairs, *before)


def output_kernel(where, own, other, w_mine, w_send, got, swapped, mine, send):
    first = jnp.where(where[2] == 0, got[...], swapped[...])
    second = jnp.where(where[2] == 0, swapped[...], got[...])

    def both(a, b):
        x = jnp.dot(own[...], a, preferred_element_type=jnp.float32).astype(jnp.bfloat16)
        y = jnp.dot(other[...], b, preferred_element_type=jnp.float32).astype(jnp.bfloat16)
        return x.astype(jnp.float32) + y.astype(jnp.float32)

    send[...] = both(w_send[...], second).astype(jnp.bfloat16)
    mine[...] = both(w_mine[...], first)


def output(where, own, other, w_out, got, swapped):
    rows, depth = own.shape
    block = got.shape[1]
    whole = lambda a: pl.BlockSpec(a.shape, lambda i, o: (0, 0))
    grid_spec = pltpu.PrefetchScalarGridSpec(
        num_scalar_prefetch=1,
        grid=(1,),
        in_specs=[whole(own), whole(other)]
        + [pl.BlockSpec((depth, block), lambda i, o, k=k: (0, o[k])) for k in (0, 1)]
        + [whole(got), whole(swapped)],
        out_specs=[pl.BlockSpec((rows, block), lambda i, o: (0, 0)) for _ in range(2)],
    )
    return pl.pallas_call(
        output_kernel,
        grid_spec=grid_spec,
        out_shape=[
            jax.ShapeDtypeStruct((rows, block), jnp.float32),
            jax.ShapeDtypeStruct((rows, block), jnp.bfloat16),
        ],
        compiler_params=VMEM,
        cost_estimate=pl.CostEstimate(
            flops=8 * rows * depth * block, transcendentals=0, bytes_accessed=10 * depth * block
        ),
        name="output",
    )(where, own, other, w_out, w_out, got, swapped)


def shards(
    hidden_in, w_query, w_key, w_value, w_pos, w_out, bias_content, bias_pos, norm_gain, norm_bias
):
    seg, block = hidden_in.shape
    model_width = w_query.shape[0]
    span = 3 * seg
    tp = lax.axis_size("tp")
    seqs = lax.axis_size("seq")
    assert tp == 4 and seqs % 2 == 0
    place = lax.axis_index("seq").astype(jnp.int32)
    rank = lax.axis_index("tp").astype(jnp.int32)
    core = place % 2
    half = seg // 2

    def across(x, k):
        return lax.ppermute(x, "tp", [(i, i ^ k) for i in range(tp)])

    def later(x, k):
        return lax.ppermute(x, "seq", [(i, i + k) for i in range(seqs - k)])

    def after(x, *others):
        return lax.optimization_barrier((x,) + others)[0]

    rel = relative(span, w_pos)

    halves = [hidden_in[:half], hidden_in[half:]]
    gathered = []
    for h in halves:
        x = after(h, gathered[0][2], rel) if gathered else h
        two = across(x, 2)
        one = across(x, 1)
        near = lax.ppermute(x, "tp", [(1, 2), (2, 1)])
        relay = lax.ppermute(two, "tp", [(1, 0), (2, 3)])
        gathered.append((h, one, two, near, relay))

    foreign = lax.dynamic_slice_in_dim(w_out, (rank ^ 2 ^ core) * block, block, 1)
    foreign = after(foreign, gathered[1][4])
    got = across(foreign, 2)
    swapped = lax.ppermute(got, "seq", [(i, i ^ 1) for i in range(seqs)])

    spot = place.reshape(1)
    query, pairs, early = [], [], []
    for g in gathered:
        q, kv = project(rank.reshape(1), g, (w_query, w_key, w_value))
        query.append(q)
        pairs.append(kv)
        early.append([later(kv, d) for d in (2, 1)])
    state = attend(
        spot, query, bias_content, bias_pos, rel,
        early[0] + pairs,
        (0, seg, 2 * seg, 2 * seg + half), 0, seg,
    )
    where = jnp.stack([rank, rank ^ 1, core])
    summed = []
    for i in range(2):
        attended = attend(
            spot, query[i : i + 1], bias_content, bias_pos, rel,
            early[1],
            (half, seg + half), i * half, seg,
            before=state,
        )
        other = across(attended, 2)
        mine, send = output(where, attended, other, w_out, got, swapped)
        received = across(send, 1)
        summed.append(halves[i].astype(jnp.float32) + mine + received.astype(jnp.float32))
    summed = jnp.concatenate(summed, 0)
    total = jnp.sum(summed, axis=1)
    center = total / block
    centred = summed - center[:, None]
    spread = jnp.sum(centred * centred, axis=1)
    stats = jnp.stack([center, spread])
    stats = [stats] + [across(stats, k) for k in range(1, tp)]
    mean = sum(s[0] for s in stats) / tp
    spread = sum(s[1] + block * (s[0] - mean) ** 2 for s in stats) / model_width
    normed = (summed - mean[:, None]) / jnp.sqrt(spread[:, None] + 1e-05)
    return (normed * norm_gain[None] + norm_bias[None]).astype(jnp.bfloat16)


def solution(mesh):
    in_specs = (
        P("seq", "tp"),
        P(None, "tp"),
        P(None, "tp"),
        P(None, "tp"),
        P(None, "tp"),
        P("tp", None),
        P("tp", None),
        P("tp", None),
        P("tp"),
        P("tp"),
    )
    out_specs = P("seq", "tp")
    return jax.shard_map(shards, mesh=mesh, in_specs=in_specs, out_specs=out_specs, check_vma=False)
```

```python
import functools

import jax
import jax.numpy as jnp
from jax import lax
from jax.experimental import pallas as pl
from jax.experimental.pallas import tpu as pltpu
from jax.sharding import PartitionSpec as P


TILE = 128
ROWS = 256
HP = 2


def limit(mib):
    return pltpu.CompilerParams(vmem_limit_bytes=mib * 2**20)


NT = (((1,), (1,)), ((), ()))
LOW = -1e30


def angles(distance, width):
    half = width // 2
    freq = jnp.exp(-jnp.log(10000.0) * jnp.arange(half).astype(jnp.float32) / half)
    angle = distance.astype(jnp.float32)[:, None] * freq[None, :]
    return jnp.sin(angle), jnp.cos(angle)


def relative_kernel(far_sin, far_cos, near_sin, near_cos, weight, out):
    block = pl.program_id(0)
    fs = far_sin[pl.ds(block, 1), :]
    fc = far_cos[pl.ds(block, 1), :]
    ns = near_sin[...]
    nc = near_cos[...]
    sin = (fs * nc + fc * ns).astype(jnp.bfloat16)
    cos = (fc * nc - fs * ns).astype(jnp.bfloat16)
    emb = jnp.concatenate([sin, cos], 1)
    out[...] = jnp.dot(emb, weight[...], preferred_element_type=jnp.float32).astype(jnp.bfloat16)


def relative(span, w_pos):
    model_width, width = w_pos.shape
    blocks = span // TILE
    far_sin, far_cos = angles(span - TILE - TILE * jnp.arange(blocks), model_width)
    near_sin, near_cos = angles(TILE - 1 - jnp.arange(TILE), model_width)
    whole = lambda a: pl.BlockSpec(a.shape, lambda b: (0, 0))
    return pl.pallas_call(
        relative_kernel,
        grid=(blocks,),
        in_specs=[whole(a) for a in (far_sin, far_cos, near_sin, near_cos, w_pos)],
        out_specs=pl.BlockSpec((TILE, width), lambda b: (b, 0)),
        out_shape=jax.ShapeDtypeStruct((span, width), jnp.bfloat16),
        compiler_params=limit(6),
        cost_estimate=pl.CostEstimate(
            flops=2 * span * model_width * width, transcendentals=0, bytes_accessed=4 * 2**20
        ),
        name="relative",
    )(far_sin, far_cos, near_sin, near_cos, w_pos)


def pack_kernel(order, w_q, w_k, w_v, w_out, out, foreign, done):
    step = pl.program_id(0)
    block, width = out.shape[0], w_q.shape[1]
    start = pl.multiple_of(order[step] * block, block)
    copies = [
        pltpu.make_async_copy(
            weight.at[pl.ds(start, block), :], out.at[:, i * width : (i + 1) * width], done.at[i]
        )
        for i, weight in enumerate((w_k, w_v, w_q))
    ]
    for copy in copies:
        copy.start()

    @pl.when(step == 0)
    def _():
        rows, cols = foreign.shape
        row = pl.multiple_of(order[pl.num_programs(0) + 1] * rows, rows)
        column = pl.multiple_of(order[pl.num_programs(0)] * cols, cols)
        extra = pltpu.make_async_copy(
            w_out.at[pl.ds(row, rows), pl.ds(column, cols)], foreign, done.at[3]
        )
        extra.start()
        extra.wait()

    for copy in copies:
        copy.wait()


def pack(order, weights, w_out, block):
    depth, width = weights[0].shape
    rows = w_out.shape[0] // 2
    grid_spec = pltpu.PrefetchScalarGridSpec(
        num_scalar_prefetch=1,
        grid=(depth // block,),
        in_specs=[pl.BlockSpec(memory_space=pltpu.HBM) for _ in range(4)],
        out_specs=[
            pl.BlockSpec((block, 3 * width), lambda k, o: (k, 0)),
            pl.BlockSpec((rows, block), lambda k, o: (0, 0)),
        ],
        scratch_shapes=[pltpu.SemaphoreType.DMA((4,))],
    )
    return pl.pallas_call(
        pack_kernel,
        grid_spec=grid_spec,
        out_shape=[
            jax.ShapeDtypeStruct((depth, 3 * width), jnp.bfloat16),
            jax.ShapeDtypeStruct((rows, block), jnp.bfloat16),
        ],
        compiler_params=limit(10),
        cost_estimate=pl.CostEstimate(
            flops=2 * 10**9, transcendentals=0, bytes_accessed=12 * depth * width
        ),
        name="pack",
    )(order, *weights, w_out)


def project_kernel(own, one, two, *refs):
    *three, w_k, w_v, w_q, query, pairs = refs
    last = three[0][...]
    if len(three) > 1:
        last = last + three[1][...]
    hidden = jnp.concatenate([own[...], one[...], two[...], last], 1)
    cols = query.shape[1]
    for weight, out in (
        (w_k, pairs.at[:, :cols]),
        (w_v, pairs.at[:, cols:]),
        (w_q, query),
    ):
        total = jnp.dot(hidden, weight[...], preferred_element_type=jnp.float32)
        out[...] = total.astype(jnp.bfloat16)


def project(hidden, packed, steps=2):
    rows, block = hidden[0].shape
    depth = packed.shape[0]
    width = packed.shape[1] // 3
    cols = width // steps
    return pl.pallas_call(
        project_kernel,
        grid=(steps,),
        in_specs=[pl.BlockSpec((rows, block), lambda n: (0, 0)) for _ in hidden]
        + [pl.BlockSpec((depth, cols), lambda n, i=i: (0, i * steps + n)) for i in range(3)],
        out_specs=[
            pl.BlockSpec((rows, cols), lambda n: (0, n)),
            pl.BlockSpec((rows, 2 * cols), lambda n: (0, n)),
        ],
        out_shape=[
            jax.ShapeDtypeStruct((rows, width), jnp.bfloat16),
            jax.ShapeDtypeStruct((rows, 2 * width), jnp.bfloat16),
        ],
        compiler_params=limit(11),
        cost_estimate=pl.CostEstimate(
            flops=6 * rows * depth * width, transcendentals=0, bytes_accessed=6 * depth * width
        ),
        name="project",
    )(*hidden, packed, packed, packed)


def attend_kernel(
    place, bias_c, bias_p, rel, *refs, first, count, pieces, seg, final, head_dim
):
    queries = refs[:count]
    pairs = refs[count : count + len(pieces)]
    refs = refs[count + len(pieces) :]
    wide = HP * head_dim
    log2 = 1.4426950408889634 / head_dim**0.5
    lane = lax.broadcasted_iota(jnp.int32, (ROWS, head_dim), 1)
    for local in range(HP):
        head = pl.program_id(0) * HP + local
        mine = slice(local * head_dim, (local + 1) * head_dim)
        theirs = slice(wide + local * head_dim, wide + (local + 1) * head_dim)
        content_bias = bias_c[pl.ds(head, 1), :]
        pos_bias = bias_p[pl.ds(head, 1), :]
        for block, q in enumerate(queries):
            here = slice(block * ROWS, (block + 1) * ROWS)
            top = first + block * ROWS
            end = 2 * seg + top + ROWS
            rows = q[:, mine].astype(jnp.float32)
            content_q = (rows + content_bias).astype(jnp.bfloat16)
            pos_q = (rows + pos_bias).astype(jnp.bfloat16)
            scores = []
            used = []
            for part, start in enumerate(pieces):
                width = min(pairs[part].shape[0], end - start)
                if width <= 0:
                    continue
                edge = start + width == end
                window = width if edge else width + ROWS
                low = seg - ROWS - top + start
                position = lax.dot_general(
                    pos_q, rel[low : low + window, mine], NT, preferred_element_type=jnp.float32
                )
                position = pltpu.roll(position, window - (ROWS - 1), 1, stride=1, stride_axis=0)
                content = lax.dot_general(
                    content_q, pairs[part][:width, mine], NT, preferred_element_type=jnp.float32
                )
                score = content + position[:, :width]
                back = 2 - start // seg
                if back > 0:
                    score = score + jnp.where(place[0] >= back, jnp.float32(0.0), jnp.float32(LOW))
                if edge:
                    row = lax.broadcasted_iota(jnp.int32, (ROWS, ROWS), 0)
                    col = lax.broadcasted_iota(jnp.int32, (ROWS, ROWS), 1)
                    tail = jnp.where(col <= row, score[:, width - ROWS :], jnp.float32(LOW))
                    score = tail if width == ROWS else jnp.concatenate([score[:, :-ROWS], tail], 1)
                scores.append(score)
                used.append((part, width))
            score = jnp.concatenate(scores, 1)
            peak = jnp.max(score, axis=1, keepdims=True)
            if final:
                before = refs[0][here, mine]
                old_peak = before[:, :1]
                old_total = before[:, head_dim // 2 : head_dim // 2 + 1]
                peak = jnp.maximum(peak, old_peak)
                keep = jnp.exp2((old_peak - peak) * log2)
            weight = jnp.exp2((score - peak) * log2)
            total = jnp.sum(weight, axis=1, keepdims=True)
            if final:
                total = total + old_total * keep
                scale = 1.0 / total
                weight = weight * scale
                result = refs[1][here, mine] * (keep * scale)
            else:
                result = None
            probs = weight.astype(jnp.bfloat16)
            start = 0
            for part, width in used:
                piece = jnp.dot(
                    probs[:, start : start + width],
                    pairs[part][:width, theirs],
                    preferred_element_type=jnp.float32,
                )
                result = piece if result is None else result + piece
                start += width
            if final:
                refs[2][here, mine] = result.astype(jnp.bfloat16)
            else:
                refs[0][here, mine] = jnp.where(lane < head_dim // 2, peak, total)
                refs[1][here, mine] = result


def attend(place, queries, bias_c, bias_p, rel, pairs, pieces, first, seg, before=()):
    heads, head_dim = bias_c.shape
    rows = len(queries) * ROWS
    wide = HP * head_dim
    final = len(before) > 0
    column = lambda n: pl.BlockSpec((n, wide), lambda h, p: (0, h))
    whole = pl.BlockSpec((heads, head_dim), lambda h, p: (0, 0))
    shape = lambda kind: jax.ShapeDtypeStruct((rows, heads * head_dim), kind)
    grid_spec = pltpu.PrefetchScalarGridSpec(
        num_scalar_prefetch=1,
        grid=(heads // HP,),
        in_specs=[whole, whole, column(3 * seg)]
        + [column(ROWS) for _ in queries]
        + [pl.BlockSpec((n.shape[0], 2 * wide), lambda h, p: (0, h)) for n in pairs]
        + [pl.BlockSpec((rows, wide), lambda h, p: (first // rows, h)) for _ in before],
        out_specs=column(rows) if final else [column(rows), column(rows)],
    )
    size = sum(k.shape[0] for k in pairs)
    return pl.pallas_call(
        functools.partial(
            attend_kernel,
            first=first,
            count=len(queries),
            pieces=pieces,
            seg=seg,
            final=final,
            head_dim=head_dim,
        ),
        grid_spec=grid_spec,
        out_shape=shape(jnp.bfloat16) if final else [shape(jnp.float32), shape(jnp.float32)],
        compiler_params=limit(8 if final else 12),
        cost_estimate=pl.CostEstimate(
            flops=16 * rows * size * heads * head_dim,
            transcendentals=rows * size * heads,
            bytes_accessed=6 * size * heads * head_dim,
        ),
        name="finish" if final else "begin",
    )(place, bias_c, bias_p, rel, *queries, *pairs, *before)


def output_kernel(where, own, other, w_mine, w_send, got, far, mine, send):
    half = got.shape[1]

    def partner(which):
        near = jnp.where(where[2] == which, got[0], far[0])
        away = jnp.where(where[2] == which, got[1], far[1])
        top = jnp.where(where[3] == 0, near, away)
        low = jnp.where(where[3] == 0, away, near)
        return jnp.dot(
            other[:, :half], top, preferred_element_type=jnp.float32
        ) + jnp.dot(other[:, half:], low, preferred_element_type=jnp.float32)

    def both(weight, which):
        x = jnp.dot(own[...], weight[...], preferred_element_type=jnp.float32)
        y = partner(which)
        return x.astype(jnp.bfloat16).astype(jnp.float32) + y.astype(jnp.bfloat16).astype(
            jnp.float32
        )

    send[...] = both(w_send, 1).astype(jnp.bfloat16)
    mine[...] = both(w_mine, 0)


def output(where, own, other, w_out, got, far):
    rows, depth = own.shape
    block = got.shape[2]
    whole = lambda a: pl.BlockSpec(a.shape, lambda i, o: (0,) * len(a.shape))
    grid_spec = pltpu.PrefetchScalarGridSpec(
        num_scalar_prefetch=1,
        grid=(1,),
        in_specs=[whole(own), whole(other)]
        + [pl.BlockSpec((depth, block), lambda i, o, k=k: (0, o[k])) for k in (0, 1)]
        + [whole(got), whole(far)],
        out_specs=[pl.BlockSpec((rows, block), lambda i, o: (0, 0)) for _ in range(2)],
    )
    return pl.pallas_call(
        output_kernel,
        grid_spec=grid_spec,
        out_shape=[
            jax.ShapeDtypeStruct((rows, block), jnp.float32),
            jax.ShapeDtypeStruct((rows, block), jnp.bfloat16),
        ],
        compiler_params=limit(8),
        cost_estimate=pl.CostEstimate(
            flops=8 * rows * depth * block, transcendentals=0, bytes_accessed=10 * depth * block
        ),
        name="output",
    )(where, own, other, w_out, w_out, got, far)


def shards(
    hidden_in, w_query, w_key, w_value, w_pos, w_out, bias_content, bias_pos, norm_gain, norm_bias
):
    seg, block = hidden_in.shape
    model_width = w_query.shape[0]
    span = 3 * seg
    tp = lax.axis_size("tp")
    seqs = lax.axis_size("seq")
    assert tp == 4 and seqs % 8 == 0
    place = lax.axis_index("seq").astype(jnp.int32)
    rank = lax.axis_index("tp").astype(jnp.int32)
    core = place % 2
    half = seg // 2
    order = jnp.bitwise_xor(rank, jnp.arange(tp, dtype=jnp.int32))
    side = (place // 4) % 2
    order = jnp.concatenate([order, jnp.stack([rank ^ 2 ^ core, side])])
    where = jnp.stack([rank, rank ^ 1, core, side])
    first_core = jnp.full((1, 2 * bias_content.size), core == 0).astype(jnp.bfloat16)
    spot = place.reshape(1)
    hidden_in, order, where, first_core, spot = lax.optimization_barrier(
        (hidden_in, order, where, first_core, spot)
    )

    def across(x, k):
        return lax.ppermute(x, "tp", [(i, i ^ k) for i in range(tp)])

    def swap(x):
        return lax.ppermute(x, "seq", [(i, i ^ 1) for i in range(seqs)])

    def after(x, *others):
        return lax.optimization_barrier((x,) + others)[0]

    halves = [hidden_in[:half], hidden_in[half:]]
    gathered = []
    for tag, h in zip("ab", halves):
        two = across(h, 2)
        one = across(h, 1)
        if tag == "a":
            near = lax.ppermute(h, "tp", [(1, 2), (2, 1)])
            relay = lax.ppermute(two, "tp", [(1, 0), (2, 3)])
            gathered.append((h, one, two, near, relay))
        else:
            gathered.append((h, one, two, across(h, 3)))

    packed, foreign = pack(order, (w_query, w_key, w_value), w_out, block)
    rel = relative(span, w_pos)

    got = across(foreign, 2)
    got = jnp.stack([got, lax.ppermute(got, "seq", [(i, i ^ 4) for i in range(seqs)])])
    far = swap(got)

    query, pairs, back = [], [], []
    for tag, g in zip("ab", gathered):
        q, kv = project(g, packed)
        query.append(q)
        pairs.append(kv)
        back.append(lax.ppermute(kv, "seq", [(i, i + 2) for i in range(seqs - 2)]))

    def last(kv, back, mask):
        return swap(jnp.where(mask > 0.5, kv, back))

    before = [back[0], last(pairs[0], back[0], first_core)]
    state = attend(
        spot, query, bias_content, bias_pos, rel,
        before + pairs,
        (0, seg, 2 * seg, 2 * seg + half), 0, seg,
    )
    first_core = after(first_core, *state)
    before = [back[1], last(pairs[1], back[1], first_core)]
    summed = []
    for i, tag in enumerate("ab"):
        attended = attend(
            spot, query[i : i + 1], bias_content, bias_pos, rel,
            before,
            (half, seg + half), i * half, seg,
            before=state,
        )
        other = across(attended, 2)
        mine, theirs = output(where, attended, other, w_out, got, far)
        received = across(theirs, 1)
        summed.append(halves[i].astype(jnp.float32) + mine + received.astype(jnp.float32))
    summed = jnp.concatenate(summed, 0)
    total = jnp.sum(summed, axis=1)
    center = total / block
    centred = summed - center[:, None]
    spread = jnp.sum(centred * centred, axis=1)
    stats = jnp.stack([center, spread])
    stats = [stats] + [across(stats, k) for k in range(1, tp)]
    mean = sum(s[0] for s in stats) / tp
    spread = sum(s[1] + block * (s[0] - mean) ** 2 for s in stats) / model_width
    normed = (summed - mean[:, None]) / jnp.sqrt(spread[:, None] + 1e-05)
    return (normed * norm_gain[None] + norm_bias[None]).astype(jnp.bfloat16)


def solution(mesh):
    in_specs = (
        P("seq", "tp"),
        P(None, "tp"),
        P(None, "tp"),
        P(None, "tp"),
        P(None, "tp"),
        P("tp", None),
        P("tp", None),
        P("tp", None),
        P("tp"),
        P("tp"),
    )
    out_specs = P("seq", "tp")

    return jax.shard_map(shards, mesh=mesh, in_specs=in_specs, out_specs=out_specs, check_vma=False)
```

```python
import functools

import jax
import jax.numpy as jnp
from jax import lax
from jax.experimental import pallas as pl
from jax.experimental.pallas import tpu as pltpu
from jax.sharding import PartitionSpec as P


TILE = 128
ROWS = 256
HP = 2


def limit(mib):
    return pltpu.CompilerParams(vmem_limit_bytes=mib * 2**20)


NT = (((1,), (1,)), ((), ()))
LOW = -1e30


def angles(distance, width):
    half = width // 2
    freq = jnp.exp(-jnp.log(10000.0) * jnp.arange(half).astype(jnp.float32) / half)
    angle = distance.astype(jnp.float32)[:, None] * freq[None, :]
    return jnp.sin(angle), jnp.cos(angle)


def relative_kernel(far_sin, far_cos, near_sin, near_cos, weight, out):
    block = pl.program_id(0)
    fs = far_sin[pl.ds(block, 1), :]
    fc = far_cos[pl.ds(block, 1), :]
    ns = near_sin[...]
    nc = near_cos[...]
    sin = (fs * nc + fc * ns).astype(jnp.bfloat16)
    cos = (fc * nc - fs * ns).astype(jnp.bfloat16)
    emb = jnp.concatenate([sin, cos], 1)
    out[...] = jnp.dot(emb, weight[...], preferred_element_type=jnp.float32).astype(jnp.bfloat16)


def relative(span, w_pos):
    model_width, width = w_pos.shape
    blocks = span // TILE
    far_sin, far_cos = angles(span - TILE - TILE * jnp.arange(blocks), model_width)
    near_sin, near_cos = angles(TILE - 1 - jnp.arange(TILE), model_width)
    whole = lambda a: pl.BlockSpec(a.shape, lambda b: (0, 0))
    return pl.pallas_call(
        relative_kernel,
        grid=(blocks,),
        in_specs=[whole(a) for a in (far_sin, far_cos, near_sin, near_cos, w_pos)],
        out_specs=pl.BlockSpec((TILE, width), lambda b: (b, 0)),
        out_shape=jax.ShapeDtypeStruct((span, width), jnp.bfloat16),
        compiler_params=limit(6),
        cost_estimate=pl.CostEstimate(
            flops=2 * span * model_width * width, transcendentals=0, bytes_accessed=4 * 2**20
        ),
        name="relative",
    )(far_sin, far_cos, near_sin, near_cos, w_pos)


def pack_kernel(order, w_q, w_k, w_v, w_out, out, foreign, done):
    step = pl.program_id(0)
    block, width = out.shape[0], w_q.shape[1]
    start = pl.multiple_of(order[step] * block, block)
    copies = [
        pltpu.make_async_copy(
            weight.at[pl.ds(start, block), :], out.at[:, i * width : (i + 1) * width], done.at[i]
        )
        for i, weight in enumerate((w_k, w_v, w_q))
    ]
    for copy in copies:
        copy.start()

    @pl.when(step == 0)
    def _():
        rows, cols = foreign.shape
        row = pl.multiple_of(order[pl.num_programs(0) + 1] * rows, rows)
        column = pl.multiple_of(order[pl.num_programs(0)] * cols, cols)
        extra = pltpu.make_async_copy(
            w_out.at[pl.ds(row, rows), pl.ds(column, cols)], foreign, done.at[3]
        )
        extra.start()
        extra.wait()

    for copy in copies:
        copy.wait()


def pack(order, weights, w_out, block):
    depth, width = weights[0].shape
    rows = w_out.shape[0] // 2
    grid_spec = pltpu.PrefetchScalarGridSpec(
        num_scalar_prefetch=1,
        grid=(depth // block,),
        in_specs=[pl.BlockSpec(memory_space=pltpu.HBM) for _ in range(4)],
        out_specs=[
            pl.BlockSpec((block, 3 * width), lambda k, o: (k, 0)),
            pl.BlockSpec((rows, block), lambda k, o: (0, 0)),
        ],
        scratch_shapes=[pltpu.SemaphoreType.DMA((4,))],
    )
    return pl.pallas_call(
        pack_kernel,
        grid_spec=grid_spec,
        out_shape=[
            jax.ShapeDtypeStruct((depth, 3 * width), jnp.bfloat16),
            jax.ShapeDtypeStruct((rows, block), jnp.bfloat16),
        ],
        compiler_params=limit(10),
        cost_estimate=pl.CostEstimate(
            flops=2 * 10**9, transcendentals=0, bytes_accessed=12 * depth * width
        ),
        name="pack",
    )(order, *weights, w_out)


def project_kernel(own, one, two, *refs, count):
    three, weights, outs = refs[: -count - 1], refs[-count - 1 : -1], refs[-1:]
    last = three[0][...]
    if len(three) > 1:
        last = last + three[1][...]
    hidden = jnp.concatenate([own[...], one[...], two[...], last], 1)
    cols = weights[0].shape[1]
    for i, weight in enumerate(weights):
        total = jnp.dot(hidden, weight[...], preferred_element_type=jnp.float32)
        out = outs[0] if count == 1 else outs[0].at[:, i * cols : (i + 1) * cols]
        out[...] = total.astype(jnp.bfloat16)


def project(hidden, packed, parts, steps=2):
    rows, block = hidden[0].shape
    depth = packed.shape[0]
    width = packed.shape[1] // 3
    cols = width // steps
    count = len(parts)
    return pl.pallas_call(
        functools.partial(project_kernel, count=count),
        grid=(steps,),
        in_specs=[pl.BlockSpec((rows, block), lambda n: (0, 0)) for _ in hidden]
        + [pl.BlockSpec((depth, cols), lambda n, i=i: (0, i * steps + n)) for i in parts],
        out_specs=pl.BlockSpec((rows, count * cols), lambda n: (0, n)),
        out_shape=jax.ShapeDtypeStruct((rows, count * width), jnp.bfloat16),
        compiler_params=limit(11),
        cost_estimate=pl.CostEstimate(
            flops=2 * count * rows * depth * width,
            transcendentals=0,
            bytes_accessed=2 * count * depth * width,
        ),
        name="project",
    )(*hidden, *[packed for _ in parts])


def attend_kernel(
    place, bias_c, bias_p, rel, *refs, first, count, pieces, seg, final, head_dim, group
):
    queries = refs[:count]
    pairs = refs[count : count + len(pieces)]
    refs = refs[count + len(pieces) :]
    wide = HP * head_dim
    log2 = 1.4426950408889634 / head_dim**0.5
    lane = lax.broadcasted_iota(jnp.int32, (ROWS, head_dim), 1)
    for local in range(group):
        head = pl.program_id(0) * group + local
        mine = slice(local * head_dim, (local + 1) * head_dim)
        base = local // HP * 2 * wide + local % HP * head_dim
        key = slice(base, base + head_dim)
        theirs = slice(base + wide, base + wide + head_dim)
        content_bias = bias_c[pl.ds(head, 1), :]
        pos_bias = bias_p[pl.ds(head, 1), :]
        for block, q in enumerate(queries):
            here = slice(block * ROWS, (block + 1) * ROWS)
            top = first + block * ROWS
            end = 2 * seg + top + ROWS
            rows = q[:, mine].astype(jnp.float32)
            content_q = (rows + content_bias).astype(jnp.bfloat16)
            pos_q = (rows + pos_bias).astype(jnp.bfloat16)
            scores = []
            used = []
            for part, start in enumerate(pieces):
                width = min(pairs[part].shape[0], end - start)
                if width <= 0:
                    continue
                edge = start + width == end
                window = width if edge else width + ROWS
                low = seg - ROWS - top + start
                position = lax.dot_general(
                    pos_q, rel[low : low + window, mine], NT, preferred_element_type=jnp.float32
                )
                position = pltpu.roll(position, window - (ROWS - 1), 1, stride=1, stride_axis=0)
                content = lax.dot_general(
                    content_q, pairs[part][:width, key], NT, preferred_element_type=jnp.float32
                )
                score = content + position[:, :width]
                back = 2 - start // seg
                if back > 0:
                    score = score + jnp.where(place[0] >= back, jnp.float32(0.0), jnp.float32(LOW))
                if edge:
                    row = lax.broadcasted_iota(jnp.int32, (ROWS, ROWS), 0)
                    col = lax.broadcasted_iota(jnp.int32, (ROWS, ROWS), 1)
                    tail = jnp.where(col <= row, score[:, width - ROWS :], jnp.float32(LOW))
                    score = tail if width == ROWS else jnp.concatenate([score[:, :-ROWS], tail], 1)
                scores.append(score)
                used.append((part, width))
            score = jnp.concatenate(scores, 1)
            peak = jnp.max(score, axis=1, keepdims=True)
            if final:
                before = refs[0][here, mine]
                old_peak = before[:, :1]
                old_total = before[:, head_dim // 2 : head_dim // 2 + 1]
                peak = jnp.maximum(peak, old_peak)
                keep = jnp.exp2((old_peak - peak) * log2)
            weight = jnp.exp2((score - peak) * log2)
            total = jnp.sum(weight, axis=1, keepdims=True)
            if final:
                total = total + old_total * keep
                scale = 1.0 / total
                weight = weight * scale
                result = refs[1][here, mine] * (keep * scale)
            else:
                result = None
            probs = weight.astype(jnp.bfloat16)
            start = 0
            for part, width in used:
                piece = jnp.dot(
                    probs[:, start : start + width],
                    pairs[part][:width, theirs],
                    preferred_element_type=jnp.float32,
                )
                result = piece if result is None else result + piece
                start += width
            if final:
                refs[2][here, mine] = result.astype(jnp.bfloat16)
            else:
                refs[0][here, mine] = jnp.where(lane < head_dim // 2, peak, total)
                refs[1][here, mine] = result


def attend(place, queries, bias_c, bias_p, rel, pairs, pieces, first, seg, before=()):
    heads, head_dim = bias_c.shape
    rows = len(queries) * ROWS
    final = len(before) > 0
    group = heads if final else HP
    wide = group * head_dim
    column = lambda n: pl.BlockSpec((n, wide), lambda h, p: (0, h))
    whole = pl.BlockSpec((heads, head_dim), lambda h, p: (0, 0))
    shape = lambda kind: jax.ShapeDtypeStruct((rows, heads * head_dim), kind)
    grid_spec = pltpu.PrefetchScalarGridSpec(
        num_scalar_prefetch=1,
        grid=(heads // group,),
        in_specs=[whole, whole, column(3 * seg)]
        + [column(ROWS) for _ in queries]
        + [pl.BlockSpec((n.shape[0], 2 * wide), lambda h, p: (0, h)) for n in pairs]
        + [pl.BlockSpec((rows, wide), lambda h, p: (first // rows, h)) for _ in before],
        out_specs=column(rows) if final else [column(rows), column(rows)],
    )
    size = sum(k.shape[0] for k in pairs)
    return pl.pallas_call(
        functools.partial(
            attend_kernel,
            first=first,
            count=len(queries),
            pieces=pieces,
            seg=seg,
            final=final,
            head_dim=head_dim,
            group=group,
        ),
        grid_spec=grid_spec,
        out_shape=shape(jnp.bfloat16) if final else [shape(jnp.float32), shape(jnp.float32)],
        compiler_params=limit(12),
        cost_estimate=pl.CostEstimate(
            flops=16 * rows * size * heads * head_dim,
            transcendentals=rows * size * heads,
            bytes_accessed=6 * size * heads * head_dim,
        ),
        name="finish" if final else "begin",
    )(place, bias_c, bias_p, rel, *queries, *pairs, *before)


def output_kernel(where, own, other, w_mine, w_send, got, far, mine, send):
    half = got.shape[1]

    def partner(which):
        near = jnp.where(where[2] == which, got[0], far[0])
        away = jnp.where(where[2] == which, got[1], far[1])
        top = jnp.where(where[3] == 0, near, away)
        low = jnp.where(where[3] == 0, away, near)
        return jnp.dot(
            other[:, :half], top, preferred_element_type=jnp.float32
        ) + jnp.dot(other[:, half:], low, preferred_element_type=jnp.float32)

    def both(weight, which):
        x = jnp.dot(own[...], weight[...], preferred_element_type=jnp.float32)
        y = partner(which)
        return x.astype(jnp.bfloat16).astype(jnp.float32) + y.astype(jnp.bfloat16).astype(
            jnp.float32
        )

    send[...] = both(w_send, 1).astype(jnp.bfloat16)
    mine[...] = both(w_mine, 0)


def output(where, own, other, w_out, got, far):
    rows, depth = own.shape
    block = got.shape[2]
    whole = lambda a: pl.BlockSpec(a.shape, lambda i, o: (0,) * len(a.shape))
    grid_spec = pltpu.PrefetchScalarGridSpec(
        num_scalar_prefetch=1,
        grid=(1,),
        in_specs=[whole(own), whole(other)]
        + [pl.BlockSpec((depth, block), lambda i, o, k=k: (0, o[k])) for k in (0, 1)]
        + [whole(got), whole(far)],
        out_specs=[pl.BlockSpec((rows, block), lambda i, o: (0, 0)) for _ in range(2)],
    )
    return pl.pallas_call(
        output_kernel,
        grid_spec=grid_spec,
        out_shape=[
            jax.ShapeDtypeStruct((rows, block), jnp.float32),
            jax.ShapeDtypeStruct((rows, block), jnp.bfloat16),
        ],
        compiler_params=limit(8),
        cost_estimate=pl.CostEstimate(
            flops=8 * rows * depth * block, transcendentals=0, bytes_accessed=10 * depth * block
        ),
        name="output",
    )(where, own, other, w_out, w_out, got, far)


def shards(
    hidden_in, w_query, w_key, w_value, w_pos, w_out, bias_content, bias_pos, norm_gain, norm_bias
):
    seg, block = hidden_in.shape
    model_width = w_query.shape[0]
    span = 3 * seg
    tp = lax.axis_size("tp")
    seqs = lax.axis_size("seq")
    assert tp == 4 and seqs % 8 == 0
    place = lax.axis_index("seq").astype(jnp.int32)
    rank = lax.axis_index("tp").astype(jnp.int32)
    core = place % 2
    half = seg // 2
    order = jnp.bitwise_xor(rank, jnp.arange(tp, dtype=jnp.int32))
    side = (place // 4) % 2
    order = jnp.concatenate([order, jnp.stack([rank ^ 2 ^ core, side])])
    where = jnp.stack([rank, rank ^ 1, core, side])
    first_core = jnp.full((1, 2 * bias_content.size), core == 0).astype(jnp.bfloat16)
    spot = place.reshape(1)
    hidden_in, order, where, first_core, spot = lax.optimization_barrier(
        (hidden_in, order, where, first_core, spot)
    )

    def across(x, k):
        return lax.ppermute(x, "tp", [(i, i ^ k) for i in range(tp)])

    def swap(x):
        return lax.ppermute(x, "seq", [(i, i ^ 1) for i in range(seqs)])

    def after(x, *others):
        return lax.optimization_barrier((x,) + others)[0]

    halves = [hidden_in[:half], hidden_in[half:]]
    gathered = []
    for tag, h in zip("ab", halves):
        two = across(h, 2)
        one = across(h, 1)
        if tag == "a":
            near = lax.ppermute(h, "tp", [(1, 2), (2, 1)])
            relay = lax.ppermute(two, "tp", [(1, 0), (2, 3)])
            gathered.append((h, one, two, near, relay))
        else:
            gathered.append((h, one, two, across(h, 3)))

    packed, foreign = pack(order, (w_query, w_key, w_value), w_out, block)
    rel = relative(span, w_pos)

    got = across(foreign, 2)
    got = jnp.stack([got, lax.ppermute(got, "seq", [(i, i ^ 4) for i in range(seqs)])])
    far = swap(got)

    query, pairs, back = [], [], []
    for tag, g in zip("ab", gathered):
        kv = project(g, packed, (0, 1))
        q = project(g, packed, (2,))
        query.append(q)
        pairs.append(kv)
        back.append(lax.ppermute(kv, "seq", [(i, i + 2) for i in range(seqs - 2)]))

    def last(kv, back, mask):
        return swap(jnp.where(mask > 0.5, kv, back))

    before = [back[0], last(pairs[0], back[0], first_core)]
    state = attend(
        spot, query, bias_content, bias_pos, rel,
        before + pairs,
        (0, seg, 2 * seg, 2 * seg + half), 0, seg,
    )
    first_core = after(first_core, *state)
    before = [back[1], last(pairs[1], back[1], first_core)]
    summed = []
    for i, tag in enumerate("ab"):
        attended = attend(
            spot, query[i : i + 1], bias_content, bias_pos, rel,
            before,
            (half, seg + half), i * half, seg,
            before=state,
        )
        other = across(attended, 2)
        mine, theirs = output(where, attended, other, w_out, got, far)
        received = across(theirs, 1)
        summed.append(halves[i].astype(jnp.float32) + mine + received.astype(jnp.float32))
    summed = jnp.concatenate(summed, 0)
    total = jnp.sum(summed, axis=1)
    center = total / block
    centred = summed - center[:, None]
    spread = jnp.sum(centred * centred, axis=1)
    stats = jnp.stack([center, spread])
    stats = [stats] + [across(stats, k) for k in range(1, tp)]
    mean = sum(s[0] for s in stats) / tp
    spread = sum(s[1] + block * (s[0] - mean) ** 2 for s in stats) / model_width
    normed = (summed - mean[:, None]) / jnp.sqrt(spread[:, None] + 1e-05)
    return (normed * norm_gain[None] + norm_bias[None]).astype(jnp.bfloat16)


def solution(mesh):
    in_specs = (
        P("seq", "tp"),
        P(None, "tp"),
        P(None, "tp"),
        P(None, "tp"),
        P(None, "tp"),
        P("tp", None),
        P("tp", None),
        P("tp", None),
        P("tp"),
        P("tp"),
    )
    out_specs = P("seq", "tp")

    return jax.shard_map(shards, mesh=mesh, in_specs=in_specs, out_specs=out_specs, check_vma=False)
```
